32 devices in a mesh: vc: 4 (over y, x), op: 8 (over z, core).
Axes of the slice: x: 2, y: 2, z: 4, core: 2. Of those that a mesh axis runs over, the one named last changes fastest.
Arguments:
- integrals: float32 [1024, 32768], P('op', 'vc'), may hold values from -0.046875 to 0.046875
- amplitudes: float32 [32768, 8192], P('vc', 'op'), may hold values from -6 to 6
- vir_energy: float32 [1024], P('vc'), may hold values from 1 to 10
- occ_energy: float32 [8192], P('op'), may hold values from -4 to -0.5
Outputs:
- update: float32 [1024, 8192], P('vc', 'op')
The draws below stay inside these ranges and needn't reach their ends.
All inputs are finite; a program needn't handle non-finite values.
Results may differ from the reference program's by a relative error of at most 0.000076.
Values sent between devices are 32-bit elements; how exact they have to be, the bound alone decides.
No kernel may reach another device: no remote copies, remote signals or barrier semaphores. Data moves between devices by JAX's collectives and lax.ppermute only.
A program may use at most 128 MiB of HBM per device.

```python
import math
import jax
import jax.numpy as jnp
from jax import lax

CD = 32768
AB = 1024
IJ = 8192


def spiked(values, rng, source, target, parts, factor):
    owner, partner = [(jnp.arange(values.shape[axis_at]) // (values.shape[axis_at] // parts)).reshape([-1 if axis == axis_at else 1 for axis in range(values.ndim)]) for axis_at in (source, target)]
    chosen = jax.random.permutation(rng, parts)[partner]
    strong = (owner == chosen) | (owner == (partner + parts // 2) % parts)
    return jnp.where(strong, factor * values, values)


def shard_levels(rng, extent, shards, low, top_value):
    factor_of = 1.0
    for axis_at, blocks in shards:
        steps = jax.random.uniform(jax.random.fold_in(jax.random.fold_in(rng, 6), axis_at), (blocks,), jnp.float32, low / len(shards), top_value / len(shards))
        factor_of = factor_of * jnp.repeat(jnp.exp(steps), extent[axis_at] // blocks).reshape((-1,) + (1,) * (len(extent) - 1 - axis_at))
    return factor_of


def scatter_about(own_key, extent, spread, most, cuts=(), kind=jnp.bfloat16):
    values = spread * jax.random.normal(own_key, extent, jnp.float32)
    if cuts:
        values = values * shard_levels(own_key, extent, cuts, -0.22, 0.18)
    return jnp.clip(values, -most, most).astype(kind)


def gaussian_with(own_key, shape, scale, most, shards, heavy, held_as=jnp.bfloat16):
    array = scale * jax.random.normal(own_key, shape, jnp.float32)
    if shards:
        array = array * shard_levels(own_key, shape, shards, -0.22, 0.18)
    return jnp.clip(spiked(array, jax.random.fold_in(own_key, 3), *heavy), -most, most).astype(held_as)


def setup_inputs(seed: int = 0) -> dict:
    keys = jax.random.split(jax.random.key(seed), 5)
    return {
        "integrals": gaussian_with(keys[0], (AB, CD), CD ** -0.5, 0.046875, ((0, 8), (1, 4)), (1, 0, 8, 2.0), jnp.float32),
        "amplitudes": scatter_about(keys[1], (CD, IJ), 1.0, 6.0, ((0, 4), (1, 8)), jnp.float32),
        "vir_energy": jnp.clip(jnp.exp(math.log(10.0) - 2.3025851 * jax.random.uniform(keys[2], (AB,), jnp.float32) ** shard_levels(keys[2], (AB,), ((0, 4),), -0.2, 0.2)), 1.0, 10.0),
        "occ_energy": jnp.clip(-4.0 + 3.5 * jax.random.uniform(keys[3], (IJ,), jnp.float32) ** shard_levels(keys[3], (IJ,), ((0, 8),), -0.2, 0.2), -4.0, -0.5),
    }


def reference(integrals, amplitudes, vir_energy, occ_energy):
    ladder = jnp.dot(integrals, amplitudes, precision=lax.Precision.HIGHEST, preferred_element_type=jnp.float32)
    return ladder / (occ_energy[None, :] - vir_energy[:, None])
```

```python
import jax
import jax.numpy as jnp
from jax import lax
from jax.sharding import PartitionSpec as P

CHUNKS = 4


def solution(mesh):
    vc, op = mesh.shape["vc"], mesh.shape["op"]

    def shards(integrals, amplitudes, vir_energy, occ_energy):
        rows = integrals.shape[0] // CHUNKS
        cols = amplitudes.shape[1]
        pieces = []
        for c in range(CHUNKS):
            part = lax.slice_in_dim(integrals, c * rows, (c + 1) * rows, axis=0)
            whole = lax.all_gather(part, "op", axis=0, tiled=True)
            partial_sum = jnp.dot(
                whole,
                amplitudes,
                precision=lax.Precision.HIGH,
                preferred_element_type=jnp.float32,
            )
            mine = lax.psum_scatter(partial_sum, "vc", scatter_dimension=0, tiled=True)
            pieces.append(mine.reshape(op // vc, rows, cols))
        ladder = jnp.concatenate(pieces, axis=1).reshape(-1, cols)
        return ladder / (occ_energy[None, :] - vir_energy[:, None])

    placed = (P("op", "vc"), P("vc", "op"), P("vc"), P("op"))
    return jax.shard_map(
        shards, mesh=mesh, in_specs=placed, out_specs=P("vc", "op"), check_vma=False
    )
```
